32 devices in a mesh: dp: 4 (over x, core), expert: 8 (over z, y).
Axes of the slice: x: 2, y: 2, z: 4, core: 2. Of those that a mesh axis runs over, the one named last changes fastest.
Arguments:
- tokens: bfloat16 [512, 2048], P(('dp', 'expert')), may hold values from -6 to 6
- out_grad: bfloat16 [512, 2048], P(('dp', 'expert')), may hold values from -6 to 6
- expert_ids: int32 [512, 8], P(('dp', 'expert')), may hold values from 0 to 63, all different within a row; in each aligned block of 16 rows (0 to 15, 16 to 31, ...) at most 4 rows name the same one
- probs: bfloat16 [512, 8], P(('dp', 'expert')), may hold values from 0.049804688 to 0.5
- w_gate: bfloat16 [64, 2048, 384], P('expert'), may hold values from -0.125 to 0.125
- w_up: bfloat16 [64, 2048, 384], P('expert'), may hold values from -0.125 to 0.125
- w_down: bfloat16 [64, 2048, 384], P('expert'), may hold values from -0.3125 to 0.3125
Outputs:
- token_grad: bfloat16 [512, 2048], P(('dp', 'expert'))
- prob_grad: bfloat16 [512, 8], P(('dp', 'expert'))
- gate_grad: float32 [64, 2048, 384], P('expert', 'dp')
- up_grad: float32 [64, 2048, 384], P('expert', 'dp')
- down_grad: float32 [64, 2048, 384], P('expert', 'dp')
The draws below stay inside these ranges and needn't reach their ends.
Inputs may be any that keep to these rules, and one draw needn't show every extreme that they name: `expert_ids`: each row names 8 different experts. Within each aligned block of 16 rows (the rows of one device) no expert is named by more than 4 rows, and that bound is reached in some blocks.
All inputs are finite; a program needn't handle non-finite values.
Results may differ from the reference program's by a relative error of at most 0.017.
Values may be sent and summed in bfloat16 or wider, within the bound.
No kernel may reach another device: no remote copies, remote signals or barrier semaphores. Data moves between devices by JAX's collectives and lax.ppermute only.
A program may use at most 128 MiB of HBM per device.

```python
import math
import jax
import jax.numpy as jnp
import numpy as np
from jax import lax

D = 2048
FF = 384
EXPERTS = 64
TOP = 8
TOK_DEV = 16
CAP = 4
TOKENS = 512
N_DP = 4
N_EXPERT = 8


def with_spikes(values, stream_key, source, target, blocks, factor):
    owner, partner = [(jnp.arange(values.shape[axis_at]) // (values.shape[axis_at] // blocks)).reshape([-1 if axis == axis_at else 1 for axis in range(values.ndim)]) for axis_at in (source, target)]
    chosen = jax.random.permutation(stream_key, blocks)[partner]
    strong = (owner == chosen) | (owner == (partner + blocks // 2) % blocks)
    return jnp.where(strong, factor * values, values)


def levels(key, dims, cuts, smallest, largest):
    gain, own = 1.0, jax.random.fold_in(key, 6)
    for position, shards_of in cuts:
        draws = jnp.exp(jax.random.uniform(jax.random.fold_in(own, position), (shards_of,), jnp.float32, smallest / len(cuts), largest / len(cuts)))
        gain = gain * jnp.repeat(draws, dims[position] // shards_of).reshape([-1 if axis == position else 1 for axis in range(len(dims))])
    return gain


def shared_out(key, own, number, rows, number_of, top, reach, slope):
    sequence = jax.random.permutation(key, number_of)
    packed, usual = load_shares(number_of, rows * top, reach, slope, True), load_shares(number_of, rows * top, reach, slope, False)
    places = jnp.arange(number_of)

    def named(tallies, offset_by):
        used = int((tallies > 0).sum())
        fixed = max(1, used // 4)
        passed = fixed + (places - fixed + offset_by * (used - fixed)) % max(1, number_of - fixed)
        return jnp.zeros((number_of,), jnp.int32).at[sequence[jnp.where(places < fixed, places, passed)]].set(jnp.asarray(tallies, jnp.int32))

    tallies = jnp.where(number % 4 == 0, named(packed, number // 4), named(usual, number - number // 4 - 1))
    mixed = jax.random.permutation(jax.random.fold_in(own, 3), number_of)
    source_of, receiver = mixed[0:number_of // 2 * 2:2], mixed[1:number_of // 2 * 2:2]
    margin = jnp.minimum(tallies[source_of] - 1, reach - tallies[receiver]) // 2
    margin = jnp.where((source_of == sequence[0]) | (receiver == sequence[0]) | (tallies[receiver] == 0), 0, jnp.maximum(margin, 0))
    passed = jax.random.randint(jax.random.fold_in(own, 4), (number_of // 2,), 0, 1 << 20) % (margin + 1)
    tallies = tallies.at[source_of].add(-passed).at[receiver].add(passed)
    items = jnp.searchsorted(jnp.cumsum(tallies), jnp.arange(rows * top), side="right").astype(jnp.int32)
    table = items.reshape(top, rows).T
    table = table[jax.random.permutation(jax.random.fold_in(own, 1), rows)]
    offset_by = jax.random.randint(jax.random.fold_in(own, 2), (rows, 1), 0, top)
    return jnp.take_along_axis(table, (jnp.arange(top)[None, :] + offset_by) % top, axis=1)


def load_shares(amount, total, most, skew, full):
    loads = [(1 << 20) // math.isqrt(rank ** skew) + 1 for rank in range(1, amount + 1)]
    largest = most if full else min(most, max(-(-total // amount), total * loads[0] // sum(loads)))
    least = 1 if total - largest >= amount - 1 else 0
    given, rest = [largest] + [least] * (amount - 1), total - largest - least * (amount - 1)
    while rest > 0:
        movable = [i for i in range(1, amount) if given[i] < largest] or [i for i in range(1, amount) if given[i] < most]
        mass, budget = sum([loads[i] for i in movable]), rest
        for i in movable:
            more = min(most - given[i], max(1, budget * loads[i] // mass), rest)
            given[i] = given[i] + more
            rest = rest - more
    return np.array(given)


def noise(stream_key, extent, width, limit, pieces=(), held_as=jnp.bfloat16):
    entries = jax.random.normal(stream_key, extent, jnp.float32) * width
    if len(pieces) > 0:
        entries = levels(stream_key, extent, pieces, -0.22, 0.18) * entries
    return jnp.clip(entries, min=-limit, max=limit).astype(held_as)


def heavy_noise(key, extent, scale, most, pieces, heavy, held_as=jnp.bfloat16):
    drawn = scale * jax.random.normal(key, extent, jnp.float32)
    if pieces:
        drawn = drawn * levels(key, extent, pieces, -0.22, 0.18)
    return jnp.clip(with_spikes(drawn, jax.random.fold_in(key, 3), *heavy), -most, most).astype(held_as)


def setup_inputs(seed: int = 0) -> dict:
    streams_of = jax.random.split(jax.random.key(seed), 8)
    tokens = heavy_noise(streams_of[0], (TOKENS, D), 1.0, 6.0, ((0, 32),), (0, 1, 32, 2.75))
    out_grad = heavy_noise(streams_of[1], (TOKENS, D), 1.0, 6.0, ((0, 32),), (0, 1, 32, 2.75))
    expert_ids_keys = jax.random.split(jax.random.fold_in(streams_of[2], 1), TOKENS // TOK_DEV)
    expert_ids_turns = jax.random.permutation(jax.random.fold_in(streams_of[2], 3), TOKENS // TOK_DEV)
    expert_ids = jax.vmap(lambda own, number: shared_out(jax.random.fold_in(streams_of[2], 2), own, number, TOK_DEV, EXPERTS, TOP, CAP, 1))(expert_ids_keys, expert_ids_turns).reshape((TOKENS, TOP))
    probs = jnp.clip(0.049804688 + 0.4501953 * jax.random.uniform(streams_of[3], (TOKENS, TOP), jnp.float32) ** levels(streams_of[3], (TOKENS, TOP), ((0, 32),), -0.2, 0.2), 0.049804688, 0.5).astype(jnp.bfloat16)
    w_gate = noise(streams_of[4], (EXPERTS, D, FF), D ** -0.5, 0.125, ((0, 8),))
    w_up = noise(streams_of[5], (EXPERTS, D, FF), D ** -0.5, 0.125, ((0, 8),))
    w_down = noise(streams_of[6], (EXPERTS, D, FF), FF ** -0.5, 0.3125, ((0, 8),))
    return dict(tokens=tokens, out_grad=out_grad, expert_ids=expert_ids, probs=probs, w_gate=w_gate, w_up=w_up, w_down=w_down)


def slot_targets(ids):
    flat = ids.reshape(ids.shape[0], -1)
    onehot = (flat[:, :, None] == jnp.arange(EXPERTS, dtype=jnp.int32)[None, None, :]).astype(jnp.int32)
    before = jnp.cumsum(onehot, axis=1) - onehot
    place = jnp.sum(before * onehot, axis=2).astype(jnp.int32)
    return (flat * CAP + place).astype(jnp.int32)


def rounded(value):
    narrow = lax.optimization_barrier(value.astype(jnp.bfloat16))
    return narrow.astype(jnp.float32)


def expert_pass(inputs):
    rows_x, rows_dy, rows_p, weight_gate, weight_up, weight_down = inputs
    gate_pre = jnp.dot(rows_x, weight_gate, preferred_element_type=jnp.float32)
    up_pre = jnp.dot(rows_x, weight_up, preferred_element_type=jnp.float32)
    sigma = jax.nn.sigmoid(gate_pre)
    silu = gate_pre * sigma
    act = (silu * up_pre).astype(jnp.bfloat16)
    scaled = (rows_p.astype(jnp.float32)[:, None] * rows_dy.astype(jnp.float32)).astype(jnp.bfloat16)
    expert_out = jnp.dot(act, weight_down.T, preferred_element_type=jnp.float32)
    prob_back = jnp.sum(rows_dy.astype(jnp.float32) * expert_out, axis=1).astype(jnp.bfloat16)
    act_grad = jnp.dot(scaled, weight_down, preferred_element_type=jnp.float32)
    gate_back = (act_grad * up_pre * sigma * (1.0 + gate_pre * (1.0 - sigma))).astype(jnp.bfloat16)
    up_back = (act_grad * silu).astype(jnp.bfloat16)
    contrib = (jnp.dot(gate_back, weight_gate.T, preferred_element_type=jnp.float32)
               + jnp.dot(up_back, weight_up.T, preferred_element_type=jnp.float32)).astype(jnp.bfloat16)
    group_gate = rounded(jnp.dot(rows_x.T, gate_back, preferred_element_type=jnp.float32))
    group_up = rounded(jnp.dot(rows_x.T, up_back, preferred_element_type=jnp.float32))
    group_down = rounded(jnp.dot(scaled.T, act, preferred_element_type=jnp.float32))
    return contrib, prob_back, (group_gate, group_up, group_down)


def reference(tokens, out_grad, expert_ids, probs, w_gate, w_up, w_down):
    pairs = TOK_DEV * TOP
    token_of = jnp.arange(pairs, dtype=jnp.int32) // TOP
    source = jnp.arange(N_EXPERT, dtype=jnp.int32)[:, None]

    def to_experts(buffer):
        shape = buffer.shape[2:]
        grid = buffer.reshape((N_EXPERT, EXPERTS, CAP) + shape)
        grid = jnp.moveaxis(grid, 1, 0)
        return grid.reshape((EXPERTS, N_EXPERT * CAP) + shape)

    def from_experts(result):
        shape = result.shape[2:]
        grid = result.reshape((EXPERTS, N_EXPERT, CAP) + shape)
        grid = jnp.moveaxis(grid, 0, 1)
        return grid.reshape((N_EXPERT, EXPERTS * CAP) + shape)

    def group_pass(carry, group):
        group_x, group_dy, group_ids, group_p = group
        target = slot_targets(group_ids)
        rows_x = group_x[:, token_of]
        rows_dy = group_dy[:, token_of]
        buffer_x = jnp.zeros((N_EXPERT, EXPERTS * CAP, D), jnp.bfloat16).at[source, target].set(rows_x)
        buffer_dy = jnp.zeros((N_EXPERT, EXPERTS * CAP, D), jnp.bfloat16).at[source, target].set(rows_dy)
        buffer_p = jnp.zeros((N_EXPERT, EXPERTS * CAP), jnp.bfloat16).at[source, target].set(group_p.reshape(N_EXPERT, pairs))
        contrib, prob_back, grads = lax.map(expert_pass, (to_experts(buffer_x), to_experts(buffer_dy), to_experts(buffer_p), w_gate, w_up, w_down))
        contrib = from_experts(contrib)
        prob_back = from_experts(prob_back)
        picked = jnp.take_along_axis(contrib, target[:, :, None], axis=1)
        token_part = jnp.sum(picked.astype(jnp.float32).reshape(N_EXPERT, TOK_DEV, TOP, D), axis=2).astype(jnp.bfloat16)
        prob_part = jnp.take_along_axis(prob_back, target, axis=1).reshape(N_EXPERT, TOK_DEV, TOP)
        carry = tuple(total + part for total, part in zip(carry, grads))
        return carry, (token_part, prob_part)

    groups = (tokens.reshape(N_DP, N_EXPERT, TOK_DEV, D), out_grad.reshape(N_DP, N_EXPERT, TOK_DEV, D),
              expert_ids.reshape(N_DP, N_EXPERT, TOK_DEV, TOP), probs.reshape(N_DP, N_EXPERT, TOK_DEV, TOP))
    empty = jnp.zeros((EXPERTS, D, FF), jnp.float32)
    totals, outputs = lax.scan(group_pass, (empty, empty, empty), groups)
    token_grad = outputs[0].reshape(TOKENS, D)
    prob_grad = outputs[1].reshape(TOKENS, TOP)
    return token_grad, prob_grad, totals[0], totals[1], totals[2]
```

```python
import functools

import jax
import jax.numpy as jnp
from jax import lax
from jax.experimental import pallas as pl
from jax.experimental.pallas import tpu as pltpu
from jax.sharding import PartitionSpec as P


F32 = jnp.float32
BF16 = jnp.bfloat16
LANES = 128
HELD = ((2, 3, 6, 7), (4, 5, 1, 0))
BLOCKS = 8
KERNEL_VMEM = 30 * 1024 * 1024
WIDE_VMEM = 48 * 1024 * 1024
FETCH_VMEM = 12 * 1024 * 1024


def _contract(left, right, left_dim, right_dim):
    return lax.dot_general(
        left, right, (((left_dim,), (right_dim,)), ((), ())), preferred_element_type=F32
    )


def _order(size):
    earlier = lax.broadcasted_iota(jnp.int32, (size, size), 0)
    later = lax.broadcasted_iota(jnp.int32, (size, size), 1)
    return (earlier < later).astype(F32).astype(BF16)


def _select(meta_t, order, base, number, rows, top, start=0):
    named, weights = [], []
    for j in range(number):
        hit = meta_t[:top, :] == (base + lax.rem(start + j, number)).astype(F32)
        named.append(jnp.sum(jnp.where(hit, 1.0, 0.0), axis=0, keepdims=True))
        weights.append(
            jnp.sum(jnp.where(hit, meta_t[top : 2 * top, :], 0.0), axis=0, keepdims=True)
        )
    spread = jnp.concatenate(named + [named[0]] * (-number % 16), axis=0).astype(BF16)
    before = _contract(spread, order, 1, 0)
    row = lax.broadcasted_iota(jnp.int32, (rows, meta_t.shape[1]), 0).astype(F32)
    picks = []
    for j in range(number):
        slot = jnp.where(named[j] > 0.0, before[j : j + 1, :], -1.0)
        picks.append(jnp.where(row == slot, 1.0, 0.0))
    return picks, weights


def _pack_kernel(tokens, out_grad, ids_t, probs_t, packet):
    rows, width = tokens.shape
    packet[:, :width] = tokens[...]
    packet[:, width : 2 * width] = out_grad[...]
    top = ids_t.shape[0]
    meta = jnp.concatenate(
        [
            ids_t[...].astype(F32),
            probs_t[...].astype(F32),
            jnp.zeros((LANES - 2 * top, rows), F32),
        ],
        axis=0,
    )
    packet[:, 2 * width :] = meta.T.astype(BF16)


def _fetch_kernel(place, source, target, sem):
    own = target.shape[0]
    copies = [
        pltpu.make_async_copy(source.at[place[0] + j], target.at[j], sem.at[j]) for j in range(own)
    ]
    for copy in copies:
        copy.start()
    for copy in copies:
        copy.wait()


def _collect(core, sources, pieces, sems, block):
    copies = []
    for side, arrays in enumerate(sources):
        for i in range(BLOCKS // 2):
            array, index = arrays[i]
            at = lax.select(core == side, HELD[0][i], HELD[1][i]) * block
            rows = pl.ds(pl.multiple_of(at, block), block)
            for n, (columns, target) in enumerate(pieces):
                source = array.at[index, :, columns]
                copy = pltpu.make_async_copy(
                    source, target.at[rows, :], sems.at[n, side * (BLOCKS // 2) + i]
                )
                copy.start()
                copies.append(copy)
    return copies


def _hidden_kernel(place, *refs, own, rows, top, inputs, block):
    sources, (wg, wu, wd) = refs[:inputs], refs[inputs : inputs + 3]
    hidden, chosen, prob, packets, packet_sems, rows_x, rows_dy = refs[inputs + 3 :]
    _, width, ff = wg.shape
    if inputs == 1:
        arrivals = [pltpu.make_async_copy(sources[0], packets, packet_sems.at[0, 0])]
        arrivals[0].start()
    else:
        both = [[(array, i) for i in range(BLOCKS // 2)] for array in sources]
        whole = [(slice(None), packets)]
        arrivals = _collect(place[2], both, whole, packet_sems, block)
    for copy in arrivals:
        copy.wait()
    meta_t = packets[:, 2 * width :].astype(F32).T
    picks, weights = _select(meta_t, _order(packets.shape[0]), place[1], own, rows, top)
    for j in range(own):
        chosen[j * rows : (j + 1) * rows, :] = picks[j].astype(BF16)
    rows_x[...] = _contract(chosen[...], packets[:, :width], 1, 0).astype(BF16)
    rows_dy[...] = _contract(chosen[...], packets[:, width : 2 * width], 1, 0).astype(BF16)
    for j in range(own):
        at = slice(j * rows, (j + 1) * rows)
        scale = jnp.sum(picks[j] * weights[j], axis=1, keepdims=True)
        gate = _contract(rows_x[at, :], wg[j], 1, 0)
        up = _contract(rows_x[at, :], wu[j], 1, 0)
        back = _contract(rows_dy[at, :], wd[j], 1, 0)
        sigma = jax.nn.sigmoid(gate)
        silu = gate * sigma
        act = silu * up
        scaled_back = scale * back
        turned = scaled_back * up * sigma * (1.0 + gate * (1.0 - sigma))
        hidden[at, :ff] = turned.astype(BF16)
        hidden[at, ff : 2 * ff] = (scaled_back * silu).astype(BF16)
        hidden[at, 2 * ff :] = (scale * act).astype(BF16)
        score = jnp.sum(act * back, axis=1, keepdims=True)
        spread = jnp.sum(picks[j] * score, axis=0, keepdims=True)
        prob[j] = jnp.broadcast_to(spread, prob.shape[1:])


def _return_kernel(place, hidden, chosen, prob, wg, wu, keep, send, rows_out, *, own, rows, block):
    _, width, ff = wg.shape
    for j in range(own):
        at = slice(j * rows, (j + 1) * rows)
        back = _contract(hidden[at, :ff], wg[j], 1, 1)
        back = back + _contract(hidden[at, ff : 2 * ff], wu[j], 1, 1)
        rows_out[at, :] = back.astype(BF16)
    part = _contract(chosen[...], rows_out[...], 0, 0).astype(BF16)
    tokens = part.shape[0]
    lane = lax.broadcasted_iota(jnp.int32, (tokens, keep.shape[2] - width), 1)
    total = jnp.zeros(lane.shape, F32)
    for j in range(own):
        total = total + jnp.where(lane == place[1] + j, prob[j].T[:, :1], 0.0)
    total = total.astype(BF16)
    if send is None:
        for s in range(tokens // block):
            at = slice(s * block, (s + 1) * block)
            keep[s, :, :width] = part[at]
            keep[s, :, width:] = total[at]
        return
    first = place[0] == 0
    for s in range(tokens // block):
        low = slice(s * block, s * block + block // 2)
        high = slice(s * block + block // 2, (s + 1) * block)
        for value, lanes in ((part, slice(0, width)), (total, slice(width, None))):
            keep[s, :, lanes] = jnp.where(first, value[low], value[high])
            send[s, :, lanes] = jnp.where(first, value[high], value[low])


def _weights_kernel(place, *refs, local, rows, top, sets, halves, block, half, ff, inputs):
    sources, hidden = refs[:inputs], refs[inputs : inputs + sets * halves]
    rest = refs[inputs + sets * halves :]
    outs, (metas, xs, dys, sems, held, gate, up, down, in_sems, out_sems) = rest[:3], rest[3:]
    count, cols = xs.shape[1:]
    per_half = local // halves
    copies = []
    if inputs == sets:
        for s in range(sets):
            for n, (columns, target) in enumerate(
                (
                    (slice(0, cols), xs),
                    (slice(cols, 2 * cols), dys),
                    (slice(2 * cols, None), metas),
                )
            ):
                copy = pltpu.make_async_copy(
                    sources[s].at[:, columns], target.at[s], sems.at[s, n, 0]
                )
                copy.start()
                copies.append(copy)
    else:
        near, far = sources[:2], sources[2:]
        number = BLOCKS // 2
        both = [
            [[(array, i) for i in range(number)] for array in near],
            [[(far[2 * side + i % 2], i // 2) for i in range(number)] for side in range(2)],
        ]
        for s, (width, index) in enumerate(((2 * half, place[2]), (half, place[3]))):
            at = pl.multiple_of(index * cols, cols)
            pieces = (
                (pl.ds(at, cols), xs.at[s]),
                (pl.ds(pl.multiple_of(width + at, cols), cols), dys.at[s]),
                (slice(2 * width, None), metas.at[s]),
            )
            copies += _collect(place[3], both[s], pieces, sems.at[s], block)
    for at_half in range(halves):
        for s in range(sets):
            target = held.at[pl.ds(at_half * per_half, per_half), pl.ds(s * rows, rows), :]
            source = hidden[s * halves + at_half]
            copy = pltpu.make_async_copy(source, target, in_sems.at[at_half, s])
            copy.start()
            copies.append(copy)
    order = _order(count)
    for copy in copies:
        copy.wait()
    picks = []
    for s in range(sets):
        turned = metas[s].astype(F32).T
        picks.append(_select(turned, order, place[1], local, rows, top, place[0])[0])
    departures = []
    for j in range(local):
        index = lax.rem(place[0] + j, local)
        turned = []
        for source in (xs, dys):
            taken = [
                _contract(picks[s][j].astype(BF16), source[s], 1, 0).astype(BF16)
                for s in range(sets)
            ]
            turned.append(jnp.concatenate(taken, axis=0))
        for i, (buffer, left) in enumerate(
            ((gate, turned[0]), (up, turned[0]), (down, turned[1]))
        ):
            buffer[j] = _contract(left, held[j, :, i * ff : (i + 1) * ff], 0, 0)
            copy = pltpu.make_async_copy(buffer.at[j], outs[i].at[index], out_sems.at[i, j])
            copy.start()
            departures.append(copy)
    for copy in departures:
        copy.wait()


def _finish_kernel(ids_t, kept, *refs):
    *others, token_grad, prob_grad_t = refs
    total = kept[...].astype(F32)
    for other in others:
        total = total + other[...].astype(F32)
    width = token_grad.shape[1]
    token_grad[...] = total[:, :width].astype(BF16)
    score = total[:, width:].T
    expert = lax.broadcasted_iota(jnp.int32, score.shape, 0)
    found = [
        jnp.sum(jnp.where(expert == ids_t[k : k + 1, :], score, 0.0), axis=0, keepdims=True)
        for k in range(ids_t.shape[0])
    ]
    prob_grad_t[...] = jnp.concatenate(found, axis=0).astype(BF16)


def _cost(flops, nbytes):
    return pl.CostEstimate(flops=int(flops), bytes_accessed=int(nbytes), transcendentals=0)


def layer(tokens, out_grad, expert_ids, probs, w_gate, w_up, w_down):
    tok_rows, width = tokens.shape
    top = expert_ids.shape[1]
    local, _, ff = w_gate.shape
    ranks, groups = lax.axis_size("expert"), lax.axis_size("dp")
    experts = local * ranks
    slots = 2 * tok_rows * top // experts
    cols = width // groups
    paired = groups == 4 and ranks == 8 and local % 2 == 0
    pair = 2 if paired else 1
    sets = groups // pair
    own = local // pair
    count = pair * ranks * tok_rows
    rows = pair * ranks * slots
    dp, rank = lax.axis_index("dp"), lax.axis_index("expert")
    core = lax.rem(dp, pair)
    extra = -(-experts // LANES) * LANES
    devices = [(d, e) for d in range(groups) for e in range(ranks)]

    def move(value, target):
        pairs = []
        for d, e in devices:
            to = target(d, e)
            if to is not None:
                pairs.append((d * ranks + e, to[0] * ranks + to[1]))
        return lax.ppermute(value, ("dp", "expert"), pairs)

    def to_core(value):
        return move(value, lambda d, e: (d ^ 1, e))

    def to_chip(value):
        return move(value, lambda d, e: (d ^ 2, e))

    def to_rank(value, first, second):
        def target(d, e):
            off = second if d % 2 else first
            return None if off is None else (d, e ^ off)

        return move(value, target)

    first = core == 0

    vmem = pl.BlockSpec(memory_space=pltpu.VMEM)
    smem = pl.BlockSpec(memory_space=pltpu.SMEM)
    hbm = pl.BlockSpec(memory_space=pltpu.HBM)
    limit = pltpu.CompilerParams(vmem_limit_bytes=KERNEL_VMEM)
    packet = pl.pallas_call(
        _pack_kernel,
        out_shape=jax.ShapeDtypeStruct((tok_rows, 2 * width + LANES), BF16),
        in_specs=[vmem] * 4,
        out_specs=vmem,
        name="pack",
    )(tokens, out_grad, expert_ids.T, probs.T)
    half = width // sets
    if paired:
        other = to_core(packet)
        chip = jnp.where(
            first,
            jnp.concatenate([packet, other], axis=0),
            jnp.concatenate([other, packet], axis=0),
        )
        at = (1 - dp // pair) * half

        def slim(block):
            return jnp.concatenate(
                [
                    lax.dynamic_slice(block, (0, at), (block.shape[0], half)),
                    lax.dynamic_slice(block, (0, width + at), (block.shape[0], half)),
                    block[:, 2 * width :],
                ],
                axis=1,
            )

        near = to_rank(chip, 2, 4)
        side = to_rank(chip, 6, 1)
        near_side = to_rank(near, 1, 1)
        side_side = to_rank(side, 1, None)
        last_block = jnp.where(first, side_side, chip)
        far_a = to_chip(jnp.stack([slim(near), slim(side)]))
        far_b = to_chip(jnp.stack([slim(near_side), slim(last_block)]))
        held = jnp.stack([near, near_side, side, last_block])
        gathered = [held, to_core(held)]
    else:
        gathered = [lax.all_gather(packet, "expert", axis=0, tiled=True)]

    place = jnp.stack([core * own, rank * local + core * own, core]).astype(jnp.int32)
    mine = []
    for weight in (w_gate, w_up, w_down):
        mine.append(
            pl.pallas_call(
                _fetch_kernel,
                out_shape=jax.ShapeDtypeStruct((own, width, ff), BF16),
                in_specs=[smem, hbm],
                out_specs=vmem,
                scratch_shapes=[pltpu.SemaphoreType.DMA((own,))],
                compiler_params=pltpu.CompilerParams(vmem_limit_bytes=FETCH_VMEM),
                cost_estimate=_cost(width * ff * own, 4 * own * width * ff),
            )(place, weight)
        )
    block = pair * tok_rows
    hidden, chosen, prob = pl.pallas_call(
        functools.partial(
            _hidden_kernel, own=own, rows=rows, top=top, inputs=len(gathered), block=block
        ),
        out_shape=(
            jax.ShapeDtypeStruct((own * rows, 3 * ff), BF16),
            jax.ShapeDtypeStruct((own * rows, count), BF16),
            jax.ShapeDtypeStruct((own, 8, count), F32),
        ),
        in_specs=[smem] + [hbm] * len(gathered) + [vmem] * 3,
        out_specs=(vmem, vmem, vmem),
        scratch_shapes=[
            pltpu.VMEM((count, 2 * width + LANES), BF16),
            pltpu.SemaphoreType.DMA((1, BLOCKS)),
        ]
        + [pltpu.VMEM((own * rows, width), BF16)] * 2,
        compiler_params=limit,
        cost_estimate=_cost(6 * own * rows * width * ff, 6 * own * width * ff),
        name="hidden",
    )(place, *gathered, *mine)

    if paired:
        sources = gathered + [far_a, far_b, to_core(far_a), to_core(far_b)]
        hidden_far = to_chip(hidden)
        hidden_all = [hidden, to_core(hidden), hidden_far, to_core(hidden_far)]
    else:
        by_owner = gathered[0][:, : 2 * width].reshape(count, 2, groups, cols)
        by_owner = jnp.moveaxis(by_owner, 2, 0).reshape(groups, count, 2 * cols)
        moved = lax.all_to_all(by_owner, "dp", 0, 0, tiled=True)
        metas = lax.all_gather(gathered[0][:, 2 * width :], "dp", axis=0)
        sources = [jnp.concatenate([moved[s], metas[s]], axis=1) for s in range(sets)]
        spread = lax.all_gather(hidden, "dp", axis=0)
        hidden_all = [spread[s] for s in range(sets)]

    kernel = functools.partial(_return_kernel, own=own, rows=rows, block=block)
    if pair == 1:
        kernel = functools.partial(
            lambda *refs, call: call(*refs[:7], None, *refs[7:]), call=kernel
        )
    piece = jax.ShapeDtypeStruct((ranks, tok_rows, width + extra), BF16)
    parts = pl.pallas_call(
        kernel,
        out_shape=(piece,) * pair,
        in_specs=[smem] + [vmem] * 5,
        out_specs=(vmem,) * pair,
        scratch_shapes=[pltpu.VMEM((own * rows, width), BF16)],
        compiler_params=limit,
        cost_estimate=_cost(8 * own * rows * width * ff, 4 * own * width * ff),
        name="contributions",
    )(place, hidden, chosen, prob, *mine[:2])

    if paired:
        theirs = to_core(parts[1])
        summed = (parts[0].astype(F32) + theirs.astype(F32)).astype(BF16)
        back = [summed[0]]
        back += [to_rank(summed[i], i, i) for i in range(ranks - 1, 0, -1)]
    else:
        back = lax.all_to_all(parts[0], "expert", 0, 0, tiled=True)
        back = [back[i] for i in range(ranks)]
    place_all = jnp.stack([core * own, rank * local, dp, core]).astype(jnp.int32)
    shape = jax.ShapeDtypeStruct((local, cols, ff), F32)
    hidden_all = [value.reshape(own, rows, 3 * ff) for value in hidden_all]
    gate_grad, up_grad, down_grad = pl.pallas_call(
        functools.partial(
            _weights_kernel,
            local=local,
            rows=rows,
            top=top,
            sets=sets,
            halves=pair,
            block=block,
            half=half,
            ff=ff,
            inputs=len(sources),
        ),
        out_shape=(shape, shape, shape),
        in_specs=[smem] + [hbm] * (len(sources) + len(hidden_all)),
        out_specs=(hbm, hbm, hbm),
        scratch_shapes=[
            pltpu.VMEM((sets, count, LANES), BF16),
            pltpu.VMEM((sets, count, cols), BF16),
            pltpu.VMEM((sets, count, cols), BF16),
            pltpu.SemaphoreType.DMA((sets, 3, BLOCKS)),
            pltpu.VMEM((local, sets * rows, 3 * ff), BF16),
        ]
        + [pltpu.VMEM((local, cols, ff), F32)] * 3
        + [pltpu.SemaphoreType.DMA((pair, sets)), pltpu.SemaphoreType.DMA((3, local))],
        compiler_params=pltpu.CompilerParams(vmem_limit_bytes=WIDE_VMEM),
        cost_estimate=_cost(6 * local * sets * rows * cols * ff, 12 * local * cols * ff),
        name="weight_grads",
    )(place_all, *sources, *hidden_all)
    token_grad, prob_grad_t = pl.pallas_call(
        _finish_kernel,
        out_shape=(
            jax.ShapeDtypeStruct((tok_rows, width), BF16),
            jax.ShapeDtypeStruct((top, tok_rows), BF16),
        ),
        in_specs=[vmem] * (1 + len(back)),
        out_specs=(vmem, vmem),
        name="finish",
    )(expert_ids.T, *back)
    prob_grad = prob_grad_t.T
    return (token_grad, prob_grad, gate_grad, up_grad, down_grad)


def solution(mesh):
    placed = (
        P(("dp", "expert"), None),
        P(("dp", "expert"), None),
        P(("dp", "expert"), None),
        P(("dp", "expert"), None),
        P("expert", None, None),
        P("expert", None, None),
        P("expert", None, None),
    )
    return jax.shard_map(
        layer,
        mesh=mesh,
        in_specs=placed,
        out_specs=(
            P(("dp", "expert"), None),
            P(("dp", "expert"), None),
            P("expert", "dp", None),
            P("expert", "dp", None),
            P("expert", "dp", None),
        ),
        check_vma=False,
    )
```

```python
import functools

import jax
import jax.numpy as jnp
from jax import lax
from jax.experimental import pallas as pl
from jax.experimental.pallas import tpu as pltpu
from jax.sharding import PartitionSpec as P


F32 = jnp.float32
BF16 = jnp.bfloat16
LANES = 128
HELD = ((2, 0, 4, 5), (1, 3, 6, 7))
BLOCKS = 8
SPLIT = 4
KERNEL_VMEM = 20 * 1024 * 1024
WIDE_VMEM = 32 * 1024 * 1024
FETCH_VMEM = 4 * 1024 * 1024


def _contract(left, right, left_dim, right_dim):
    return lax.dot_general(
        left, right, (((left_dim,), (right_dim,)), ((), ())), preferred_element_type=F32
    )


def _order(size):
    earlier = lax.broadcasted_iota(jnp.int32, (size, size), 0)
    later = lax.broadcasted_iota(jnp.int32, (size, size), 1)
    return (earlier < later).astype(F32).astype(BF16)


def _select(meta_t, order, base, number, rows, top, start=0):
    named, weights = [], []
    for j in range(number):
        hit = meta_t[:top, :] == (base + lax.rem(start + j, number)).astype(F32)
        named.append(jnp.sum(jnp.where(hit, 1.0, 0.0), axis=0, keepdims=True))
        weights.append(
            jnp.sum(jnp.where(hit, meta_t[top : 2 * top, :], 0.0), axis=0, keepdims=True)
        )
    spread = jnp.concatenate(named + [named[0]] * (-number % 16), axis=0).astype(BF16)
    before = _contract(spread, order, 1, 0)
    row = lax.broadcasted_iota(jnp.int32, (rows, meta_t.shape[1]), 0).astype(F32)
    picks = []
    for j in range(number):
        slot = jnp.where(named[j] > 0.0, before[j : j + 1, :], -1.0)
        picks.append(jnp.where(row == slot, 1.0, 0.0))
    return picks, weights


def _pack_kernel(tokens, out_grad, ids_t, probs_t, packet):
    rows, width = tokens.shape
    packet[:, :width] = tokens[...]
    packet[:, width : 2 * width] = out_grad[...]
    top = ids_t.shape[0]
    meta = jnp.concatenate(
        [
            ids_t[...].astype(F32),
            probs_t[...].astype(F32),
            jnp.zeros((LANES - 2 * top, rows), F32),
        ],
        axis=0,
    )
    packet[:, 2 * width :] = meta.T.astype(BF16)


def _pieces(size):
    step = size // SPLIT
    return [pl.ds(n * step, step) for n in range(SPLIT)]


def _fetch_kernel(place, *refs, skip):
    *sources, target, sem = refs
    number, _, total = target.shape
    ff = total // len(sources)
    copies = []
    for j in range(number):
        for i, source in enumerate(sources):
            for n, rows in enumerate(_pieces(target.shape[1])):
                part = target.at[j, rows, pl.ds(i * ff, ff)]
                whole = source.at[place[0] + skip + j, rows, :]
                copies.append(pltpu.make_async_copy(whole, part, sem.at[i, j, n]))
    for copy in copies:
        copy.start()
    for copy in copies:
        copy.wait()


def _collect(core, sources, pieces, sems, block):
    copies = []
    for side, arrays in enumerate(sources):
        for i in range(BLOCKS // 2):
            array, index = arrays[i]
            at = lax.select(core == side, HELD[0][i], HELD[1][i]) * block
            rows = pl.ds(pl.multiple_of(at, block), block)
            for n, (columns, target) in enumerate(pieces):
                source = array.at[index, :, columns]
                copy = pltpu.make_async_copy(
                    source, target.at[rows, :], sems.at[n, side * (BLOCKS // 2) + i]
                )
                copy.start()
                copies.append(copy)
    return copies


def _hidden_kernel(place, *refs, own, rows, top, inputs, block):
    sources, weights = refs[:inputs], refs[inputs:-7]
    *wide, wd = weights
    hidden, chosen, prob, packets, packet_sems, rows_x, rows_dy = refs[-7:]
    chunk = own // len(wide)
    _, width, ff = wd.shape
    if inputs == 1:
        arrivals = [pltpu.make_async_copy(sources[0], packets, packet_sems.at[0, 0])]
        arrivals[0].start()
    else:
        both = [[(array, i) for i in range(BLOCKS // 2)] for array in sources]
        whole = [(slice(None), packets)]
        arrivals = _collect(place[2], both, whole, packet_sems, block)
    for copy in arrivals:
        copy.wait()
    meta_t = packets[:, 2 * width :].astype(F32).T
    picks, scales = _select(meta_t, _order(packets.shape[0]), place[1], own, rows, top)
    for j in range(own):
        chosen[j * rows : (j + 1) * rows, :] = picks[j].astype(BF16)
    rows_x[...] = _contract(chosen[...], packets[:, :width], 1, 0).astype(BF16)
    rows_dy[...] = _contract(chosen[...], packets[:, width : 2 * width], 1, 0).astype(BF16)
    for j in range(own):
        at = slice(j * rows, (j + 1) * rows)
        scale = jnp.sum(picks[j] * scales[j], axis=1, keepdims=True)
        both = _contract(rows_x[at, :], wide[j // chunk][j % chunk], 1, 0)
        gate, up = both[:, :ff], both[:, ff:]
        back = _contract(rows_dy[at, :], wd[j], 1, 0)
        sigma = jax.nn.sigmoid(gate)
        silu = gate * sigma
        act = silu * up
        scaled_back = scale * back
        turned = scaled_back * up * sigma * (1.0 + gate * (1.0 - sigma))
        hidden[at, :ff] = turned.astype(BF16)
        hidden[at, ff : 2 * ff] = (scaled_back * silu).astype(BF16)
        hidden[at, 2 * ff :] = (scale * act).astype(BF16)
        score = jnp.sum(act * back, axis=1, keepdims=True)
        spread = jnp.sum(picks[j] * score, axis=0, keepdims=True)
        prob[j] = jnp.broadcast_to(spread, prob.shape[1:])


def _return_kernel(place, hidden, chosen, prob, *refs, own, rows, block):
    wide = refs[: -2 if block is None else -3]
    keep, rows_out = refs[len(wide)], refs[-1]
    width, both = wide[0].shape[1:]
    chunk = own // len(wide)
    for j in range(own):
        at = slice(j * rows, (j + 1) * rows)
        back = _contract(hidden[at, :both], wide[j // chunk][j % chunk], 1, 1)
        rows_out[at, :] = back.astype(BF16)
    part = _contract(chosen[...], rows_out[...], 0, 0).astype(BF16)
    tokens = part.shape[0]
    lane = lax.broadcasted_iota(jnp.int32, (tokens, keep.shape[2] - width), 1)
    total = jnp.zeros(lane.shape, F32)
    for j in range(own):
        total = total + jnp.where(lane == place[1] + j, prob[j].T[:, :1], 0.0)
    total = total.astype(BF16)
    if block is None:
        single = keep.shape[1]
        for s in range(tokens // single):
            at = slice(s * single, (s + 1) * single)
            keep[s, :, :width] = part[at]
            keep[s, :, width:] = total[at]
        return
    first, send = place[0] == 0, refs[-2]
    for s in range(tokens // block):
        low = slice(s * block, s * block + block // 2)
        high = slice(s * block + block // 2, (s + 1) * block)
        for value, lanes in ((part, slice(0, width)), (total, slice(width, None))):
            to = place[3] ^ s
            keep[to, :, lanes] = jnp.where(first, value[low], value[high])
            send[to, :, lanes] = jnp.where(first, value[high], value[low])


def _weights_kernel(place, *refs, local, rows, top, sets, halves, block, half, ff, inputs):
    sources, hidden = refs[:inputs], refs[inputs : inputs + sets * halves]
    rest = refs[inputs + sets * halves :]
    outs, (metas, xs, dys, sems, held, gate, up, down, in_sems, out_sems) = rest[:3], rest[3:]
    count, cols = xs.shape[1:]
    per_half = local // halves
    copies = []
    if inputs == sets:
        for s in range(sets):
            for n, (columns, target) in enumerate(
                (
                    (slice(0, cols), xs),
                    (slice(cols, 2 * cols), dys),
                    (slice(2 * cols, None), metas),
                )
            ):
                copy = pltpu.make_async_copy(
                    sources[s].at[:, columns], target.at[s], sems.at[s, n, 0]
                )
                copy.start()
                copies.append(copy)
    else:
        near, far = sources[:2], sources[2:]
        number = BLOCKS // 2
        both = [
            [[(array, i) for i in range(number)] for array in near],
            [[(far[2 * side + i // 2], i % 2) for i in range(number)] for side in range(2)],
        ]
        for s, (width, index) in enumerate(((2 * half, place[2]), (half, place[3]))):
            at = pl.multiple_of(index * cols, cols)
            pieces = (
                (pl.ds(at, cols), xs.at[s]),
                (pl.ds(pl.multiple_of(width + at, cols), cols), dys.at[s]),
                (slice(2 * width, None), metas.at[s]),
            )
            copies += _collect(place[3], both[s], pieces, sems.at[s], block)
    for at_half in range(halves):
        for s in range(sets):
            target = held.at[pl.ds(at_half * per_half, per_half), pl.ds(s * rows, rows), :]
            source = hidden[s * halves + at_half]
            copy = pltpu.make_async_copy(source, target, in_sems.at[at_half, s])
            copy.start()
            copies.append(copy)
    order = _order(count)
    for copy in copies:
        copy.wait()
    picks = []
    for s in range(sets):
        turned = metas[s].astype(F32).T
        picks.append(_select(turned, order, place[1], local, rows, top, place[0])[0])
    departures = []
    for j in range(local):
        index = lax.rem(place[0] + j, local)
        turned = []
        for source in (xs, dys):
            taken = [
                _contract(picks[s][j].astype(BF16), source[s], 1, 0).astype(BF16)
                for s in range(sets)
            ]
            turned.append(jnp.concatenate(taken, axis=0))
        for i, (buffer, left) in enumerate(
            ((gate, turned[0]), (up, turned[0]), (down, turned[1]))
        ):
            buffer[j] = _contract(left, held[j, :, i * ff : (i + 1) * ff], 0, 0)
            copy = pltpu.make_async_copy(buffer.at[j], outs[i].at[index], out_sems.at[i, j])
            copy.start()
            departures.append(copy)
    for copy in departures:
        copy.wait()


def _finish_kernel(ids_t, back, token_grad, prob_grad_t):
    total = jnp.sum(back[...].astype(F32), axis=0)
    width = token_grad.shape[1]
    token_grad[...] = total[:, :width].astype(BF16)
    score = total[:, width:].T
    expert = lax.broadcasted_iota(jnp.int32, score.shape, 0)
    found = [
        jnp.sum(jnp.where(expert == ids_t[k : k + 1, :], score, 0.0), axis=0, keepdims=True)
        for k in range(ids_t.shape[0])
    ]
    prob_grad_t[...] = jnp.concatenate(found, axis=0).astype(BF16)


def _in_hbm(values):
    return [pltpu.with_memory_space_constraint(value, pltpu.HBM) for value in values]


def _cost(flops, nbytes):
    return pl.CostEstimate(flops=int(flops), bytes_accessed=int(nbytes), transcendentals=0)


def layer(tokens, out_grad, expert_ids, probs, w_gate, w_up, w_down):
    tok_rows, width = tokens.shape
    top = expert_ids.shape[1]
    local, _, ff = w_gate.shape
    ranks, groups = lax.axis_size("expert"), lax.axis_size("dp")
    experts = local * ranks
    slots = 2 * tok_rows * top // experts
    cols = width // groups
    paired = groups == 4 and ranks == 8 and local % 2 == 0
    pair = 2 if paired else 1
    sets = groups // pair
    own = local // pair
    count = pair * ranks * tok_rows
    rows = pair * ranks * slots
    dp, rank = lax.axis_index("dp"), lax.axis_index("expert")
    core = lax.rem(dp, pair)
    extra = -(-experts // LANES) * LANES
    devices = [(d, e) for d in range(groups) for e in range(ranks)]

    def move(value, target):
        pairs = []
        for d, e in devices:
            to = target(d, e)
            if to is not None:
                pairs.append((d * ranks + e, to[0] * ranks + to[1]))
        return lax.ppermute(value, ("dp", "expert"), pairs)

    def to_core(value):
        return move(value, lambda d, e: (d ^ 1, e))

    def to_chip(value):
        return move(value, lambda d, e: (d ^ 2, e))

    def to_rank(value, first, second):
        def target(d, e):
            off = second if d % 2 else first
            return None if off is None else (d, e ^ off)

        return move(value, target)

    first = core == 0

    vmem = pl.BlockSpec(memory_space=pltpu.VMEM)
    smem = pl.BlockSpec(memory_space=pltpu.SMEM)
    hbm = pl.BlockSpec(memory_space=pltpu.HBM)
    limit = pltpu.CompilerParams(vmem_limit_bytes=KERNEL_VMEM)
    packet = pl.pallas_call(
        _pack_kernel,
        out_shape=jax.ShapeDtypeStruct((tok_rows, 2 * width + LANES), BF16),
        in_specs=[vmem] * 4,
        out_specs=vmem,
        name="pack",
    )(tokens, out_grad, expert_ids.T, probs.T)
    half = width // sets
    if paired:
        other = to_core(packet)
        chip = jnp.where(
            first,
            jnp.concatenate([packet, other], axis=0),
            jnp.concatenate([other, packet], axis=0),
        )
        at = (1 - dp // pair) * half

        def slim(block):
            return jnp.concatenate(
                [
                    lax.dynamic_slice(block, (0, at), (block.shape[0], half)),
                    lax.dynamic_slice(block, (0, width + at), (block.shape[0], half)),
                    block[:, 2 * width :],
                ],
                axis=1,
            )

        near = to_rank(chip, 2, 1)
        side = to_rank(chip, 4, 6)
        near_side = jnp.where(first, chip, to_rank(near, None, 2))
        side_side = to_rank(side, 1, 1)
        far_a = to_chip(jnp.stack([slim(near), slim(near_side)]))
        far_b = to_chip(jnp.stack([slim(side), slim(side_side)]))
        held = jnp.stack([near, near_side, side, side_side])
        gathered = [held, to_core(held)]
    else:
        gathered = [lax.all_gather(packet, "expert", axis=0, tiled=True)]

    place = jnp.stack([core * own, rank * local + core * own, core, rank]).astype(jnp.int32)

    def fetch(weights, skip, number):
        shape = (number, width, len(weights) * ff)
        return pl.pallas_call(
            functools.partial(_fetch_kernel, skip=skip),
            out_shape=pltpu.VMEM(shape, BF16),
            in_specs=[smem] + [hbm] * len(weights),
            out_specs=vmem,
            scratch_shapes=[pltpu.SemaphoreType.DMA((len(weights), number, SPLIT))],
            compiler_params=pltpu.CompilerParams(vmem_limit_bytes=FETCH_VMEM),
            cost_estimate=_cost(width * ff * own, 4 * own * width * ff),
        )(place, *_in_hbm(weights))

    chunk = own // pair
    wide = [fetch((w_gate, w_up), i * chunk, chunk) for i in range(own // chunk)]
    down = fetch((w_down,), 0, own)
    block = pair * tok_rows
    hidden, chosen, prob = pl.pallas_call(
        functools.partial(
            _hidden_kernel, own=own, rows=rows, top=top, inputs=len(gathered), block=block
        ),
        out_shape=(
            jax.ShapeDtypeStruct((own * rows, 3 * ff), BF16),
            jax.ShapeDtypeStruct((own * rows, count), BF16),
            jax.ShapeDtypeStruct((own, 8, count), F32),
        ),
        in_specs=[smem] + [hbm] * len(gathered) + [vmem] * (len(wide) + 1),
        out_specs=(vmem, vmem, vmem),
        scratch_shapes=[
            pltpu.VMEM((count, 2 * width + LANES), BF16),
            pltpu.SemaphoreType.DMA((1, BLOCKS)),
        ]
        + [pltpu.VMEM((own * rows, width), BF16)] * 2,
        compiler_params=limit,
        cost_estimate=_cost(6 * own * rows * width * ff, 6 * own * width * ff),
        name="hidden",
    )(place, *gathered, *wide, down)

    if paired:
        sources = gathered + [far_a, far_b, to_core(far_a), to_core(far_b)]
        hidden_far = to_chip(hidden)
        hidden_all = [hidden, to_core(hidden), hidden_far, to_core(hidden_far)]
    else:
        by_owner = gathered[0][:, : 2 * width].reshape(count, 2, groups, cols)
        by_owner = jnp.moveaxis(by_owner, 2, 0).reshape(groups, count, 2 * cols)
        moved = lax.all_to_all(by_owner, "dp", 0, 0, tiled=True)
        metas = lax.all_gather(gathered[0][:, 2 * width :], "dp", axis=0)
        sources = [jnp.concatenate([moved[s], metas[s]], axis=1) for s in range(sets)]
        spread = lax.all_gather(hidden, "dp", axis=0)
        hidden_all = [spread[s] for s in range(sets)]

    kernel = functools.partial(
        _return_kernel, own=own, rows=rows, block=block if paired else None
    )
    piece = jax.ShapeDtypeStruct((ranks, tok_rows, width + extra), BF16)
    parts = pl.pallas_call(
        kernel,
        out_shape=(piece,) * pair,
        in_specs=[smem] + [vmem] * (3 + len(wide)),
        out_specs=(vmem,) * pair,
        scratch_shapes=[pltpu.VMEM((own * rows, width), BF16)],
        compiler_params=limit,
        cost_estimate=_cost(8 * own * rows * width * ff, 4 * own * width * ff),
        name="contributions",
    )(place, hidden, chosen, prob, *wide)

    if paired:
        theirs = to_core(parts[1])
        summed = (parts[0].astype(F32) + theirs.astype(F32)).astype(BF16)
    else:
        summed = parts[0]
    back = lax.all_to_all(summed, "expert", 0, 0, tiled=True)
    place_all = jnp.stack([core * own, rank * local, dp, core]).astype(jnp.int32)
    shape = jax.ShapeDtypeStruct((local, cols, ff), F32)
    hidden_all = [value.reshape(own, rows, 3 * ff) for value in hidden_all]
    gate_grad, up_grad, down_grad = pl.pallas_call(
        functools.partial(
            _weights_kernel,
            local=local,
            rows=rows,
            top=top,
            sets=sets,
            halves=pair,
            block=block,
            half=half,
            ff=ff,
            inputs=len(sources),
        ),
        out_shape=(shape, shape, shape),
        in_specs=[smem] + [hbm] * (len(sources) + len(hidden_all)),
        out_specs=(hbm, hbm, hbm),
        scratch_shapes=[
            pltpu.VMEM((sets, count, LANES), BF16),
            pltpu.VMEM((sets, count, cols), BF16),
            pltpu.VMEM((sets, count, cols), BF16),
            pltpu.SemaphoreType.DMA((sets, 3, BLOCKS)),
            pltpu.VMEM((local, sets * rows, 3 * ff), BF16),
        ]
        + [pltpu.VMEM((local, cols, ff), F32)] * 3
        + [pltpu.SemaphoreType.DMA((pair, sets)), pltpu.SemaphoreType.DMA((3, local))],
        compiler_params=pltpu.CompilerParams(vmem_limit_bytes=WIDE_VMEM),
        cost_estimate=_cost(6 * local * sets * rows * cols * ff, 12 * local * cols * ff),
        name="weight_grads",
    )(place_all, *sources, *hidden_all)
    token_grad, prob_grad_t = pl.pallas_call(
        _finish_kernel,
        out_shape=(
            jax.ShapeDtypeStruct((tok_rows, width), BF16),
            jax.ShapeDtypeStruct((top, tok_rows), BF16),
        ),
        in_specs=[vmem] * 2,
        out_specs=(vmem, vmem),
        name="finish",
    )(expert_ids.T, back)
    prob_grad = prob_grad_t.T
    return (token_grad, prob_grad, gate_grad, up_grad, down_grad)


def solution(mesh):
    placed = (
        P(("dp", "expert"), None),
        P(("dp", "expert"), None),
        P(("dp", "expert"), None),
        P(("dp", "expert"), None),
        P("expert", None, None),
        P("expert", None, None),
        P("expert", None, None),
    )
    return jax.shard_map(
        layer,
        mesh=mesh,
        in_specs=placed,
        out_specs=(
            P(("dp", "expert"), None),
            P(("dp", "expert"), None),
            P("expert", "dp", None),
            P("expert", "dp", None),
            P("expert", "dp", None),
        ),
        check_vma=False,
    )
```

```python
import functools

import jax
import jax.numpy as jnp
from jax import lax
from jax.experimental import pallas as pl
from jax.experimental.pallas import tpu as pltpu
from jax.sharding import PartitionSpec as P


F32 = jnp.float32
BF16 = jnp.bfloat16
LANES = 128
BLOCKS = 8
SPLIT = 4
KERNEL_VMEM = 20 * 1024 * 1024
WIDE_VMEM = 32 * 1024 * 1024
FETCH_VMEM = 4 * 1024 * 1024


def _contract(left, right, left_dim, right_dim):
    return lax.dot_general(
        left, right, (((left_dim,), (right_dim,)), ((), ())), preferred_element_type=F32
    )


def _order(size):
    earlier = lax.broadcasted_iota(jnp.int32, (size, size), 0)
    later = lax.broadcasted_iota(jnp.int32, (size, size), 1)
    return (earlier < later).astype(F32).astype(BF16)


def _select(meta_t, order, base, number, rows, top, start=0):
    named, weights = [], []
    for j in range(number):
        hit = meta_t[:top, :] == (base + lax.rem(start + j, number)).astype(F32)
        named.append(jnp.sum(jnp.where(hit, 1.0, 0.0), axis=0, keepdims=True))
        weights.append(
            jnp.sum(jnp.where(hit, meta_t[top : 2 * top, :], 0.0), axis=0, keepdims=True)
        )
    spread = jnp.concatenate(named + [named[0]] * (-number % 16), axis=0).astype(BF16)
    before = _contract(spread, order, 1, 0)
    row = lax.broadcasted_iota(jnp.int32, (rows, meta_t.shape[1]), 0).astype(F32)
    picks = []
    for j in range(number):
        slot = jnp.where(named[j] > 0.0, before[j : j + 1, :], -1.0)
        picks.append(jnp.where(row == slot, 1.0, 0.0))
    return picks, weights


def _pack_kernel(tokens, out_grad, ids_t, probs_t, packet):
    rows, width = tokens.shape
    packet[:, :width] = tokens[...]
    packet[:, width : 2 * width] = out_grad[...]
    top = ids_t.shape[0]
    meta = jnp.concatenate(
        [
            ids_t[...].astype(F32),
            probs_t[...].astype(F32),
            jnp.zeros((LANES - 2 * top, rows), F32),
        ],
        axis=0,
    )
    packet[:, 2 * width :] = meta.T.astype(BF16)


def _pieces(size):
    step = size // SPLIT
    return [pl.ds(n * step, step) for n in range(SPLIT)]


def _fetch_kernel(place, *refs, skip):
    *sources, target, sem = refs
    number, _, total = target.shape
    ff = total // len(sources)
    copies = []
    for j in range(number):
        for i, source in enumerate(sources):
            for n, rows in enumerate(_pieces(target.shape[1])):
                part = target.at[j, rows, pl.ds(i * ff, ff)]
                whole = source.at[place[0] + skip + j, rows, :]
                copies.append(pltpu.make_async_copy(whole, part, sem.at[i, j, n]))
    for copy in copies:
        copy.start()
    for copy in copies:
        copy.wait()


def _start(copies):
    for copy in copies:
        copy.start()
    return copies


def _hidden_kernel(place, *refs, own, rows, top, inputs, block):
    sources, weights = refs[:inputs], refs[inputs:-7]
    *wide, wd = weights
    hidden, chosen, prob, packets, packet_sems, rows_x, rows_dy = refs[-7:]
    chunk = own // len(wide)
    _, width, ff = wd.shape
    if inputs == 1:
        whole = packets.at[:, 0]
        arrivals = _start([pltpu.make_async_copy(sources[0], whole, packet_sems.at[0, 0])])
    else:
        arrivals = _start(
            [
                pltpu.make_async_copy(array, packets.at[:, (place[2] + i) % 2], packet_sems.at[0, i])
                for i, array in enumerate(sources)
            ]
        )
    for copy in arrivals:
        copy.wait()
    count = chosen.shape[1]
    meta_t = packets[..., 2 * width :].reshape(count, LANES).astype(F32).T
    picks, scales = _select(meta_t, _order(count), place[1], own, rows, top)
    for j in range(own):
        chosen[j * rows : (j + 1) * rows, :] = picks[j].astype(BF16)
    rows_x[...] = _contract(chosen[...], packets[..., :width].reshape(count, width), 1, 0).astype(BF16)
    grads = packets[..., width : 2 * width].reshape(count, width)
    rows_dy[...] = _contract(chosen[...], grads, 1, 0).astype(BF16)
    for j in range(own):
        at = slice(j * rows, (j + 1) * rows)
        scale = jnp.sum(picks[j] * scales[j], axis=1, keepdims=True)
        both = _contract(rows_x[at, :], wide[j // chunk][j % chunk], 1, 0)
        gate, up = both[:, :ff], both[:, ff:]
        back = _contract(rows_dy[at, :], wd[j], 1, 0)
        sigma = jax.nn.sigmoid(gate)
        silu = gate * sigma
        act = silu * up
        scaled_back = scale * back
        turned = scaled_back * up * sigma * (1.0 + gate * (1.0 - sigma))
        hidden[at, :ff] = turned.astype(BF16)
        hidden[at, ff : 2 * ff] = (scaled_back * silu).astype(BF16)
        hidden[at, 2 * ff :] = (scale * act).astype(BF16)
        score = jnp.sum(act * back, axis=1, keepdims=True)
        spread = jnp.sum(picks[j] * score, axis=0, keepdims=True)
        prob[j] = jnp.broadcast_to(spread, prob.shape[1:])


def _return_kernel(place, hidden, chosen, prob, *refs, own, rows, block):
    wide = refs[: -2 if block is None else -3]
    keep, rows_out = refs[len(wide)], refs[-1]
    width, both = wide[0].shape[1:]
    chunk = own // len(wide)
    for j in range(own):
        at = slice(j * rows, (j + 1) * rows)
        back = _contract(hidden[at, :both], wide[j // chunk][j % chunk], 1, 1)
        rows_out[at, :] = back.astype(BF16)
    part = _contract(chosen[...], rows_out[...], 0, 0).astype(BF16)
    tokens = part.shape[0]
    lane = lax.broadcasted_iota(jnp.int32, (tokens, keep.shape[2] - width), 1)
    total = jnp.zeros(lane.shape, F32)
    for j in range(own):
        total = total + jnp.where(lane == place[1] + j, prob[j].T[:, :1], 0.0)
    total = total.astype(BF16)
    if block is None:
        single = keep.shape[1]
        for s in range(tokens // single):
            at = slice(s * single, (s + 1) * single)
            keep[s, :, :width] = part[at]
            keep[s, :, width:] = total[at]
        return
    first, send = place[0] == 0, refs[-2]
    for s in range(tokens // block):
        low = slice(s * block, s * block + block // 2)
        high = slice(s * block + block // 2, (s + 1) * block)
        for value, lanes in ((part, slice(0, width)), (total, slice(width, None))):
            to = place[3] ^ s
            keep[to, :, lanes] = jnp.where(first, value[low], value[high])
            send[to, :, lanes] = jnp.where(first, value[high], value[low])


def _weights_kernel(place, *refs, local, rows, top, sets, halves, block, half, ff, inputs):
    sources, hidden = refs[:inputs], refs[inputs : inputs + sets * halves]
    rest = refs[inputs + sets * halves :]
    outs, (metas, xs, dys, sems, held, gate, up, down, in_sems, out_sems) = rest[:3], rest[3:]
    cols = xs.shape[-1]
    count = xs.shape[1] * xs.shape[2] * xs.shape[3]
    per_half = local // halves
    copies = []
    spans = []
    if inputs == sets:
        for s in range(sets):
            spans.append((sources[s], s, slice(None), 0, 0, cols, 0))
    else:
        near, far = sources[:2], sources[2:]
        for i in range(2):
            lane = (place[3] + i) % 2
            at = pl.multiple_of(place[2] * cols, cols)
            spans.append((near[i], 0, slice(None), lane, at, 2 * half, i))
            at = pl.multiple_of(place[3] * cols, cols)
            for part in range(2):
                blocks = pl.ds(part * BLOCKS // 2, BLOCKS // 2)
                spans.append((far[2 * i + part], 1, blocks, lane, at, half, 2 * i + part))
    for source, s, blocks, lane, at, span, sem in spans:
        pieces = (
            (pl.ds(at, cols), xs),
            (pl.ds(pl.multiple_of(span + at, cols), cols), dys),
            (slice(2 * span, None), metas),
        )
        for n, (columns, target) in enumerate(pieces):
            to = target.at[s, blocks, lane]
            copy = pltpu.make_async_copy(source.at[:, :, columns], to, sems.at[s, n, sem])
            copy.start()
            copies.append(copy)
    for at_half in range(halves):
        for s in range(sets):
            target = held.at[pl.ds(at_half * per_half, per_half), pl.ds(s * rows, rows), :]
            source = hidden[s * halves + at_half]
            copy = pltpu.make_async_copy(source, target, in_sems.at[at_half, s])
            copy.start()
            copies.append(copy)
    order = _order(count)
    for copy in copies:
        copy.wait()
    picks = []
    for s in range(sets):
        turned = metas[s].reshape(count, LANES).astype(F32).T
        picks.append(_select(turned, order, place[1], local, rows, top, place[0])[0])
    departures = []
    for j in range(local):
        index = lax.rem(place[0] + j, local)
        turned = []
        for source in (xs, dys):
            taken = [
                _contract(picks[s][j].astype(BF16), source[s].reshape(count, cols), 1, 0).astype(BF16)
                for s in range(sets)
            ]
            turned.append(jnp.concatenate(taken, axis=0))
        for i, (buffer, left) in enumerate(
            ((gate, turned[0]), (up, turned[0]), (down, turned[1]))
        ):
            buffer[j] = _contract(left, held[j, :, i * ff : (i + 1) * ff], 0, 0)
            copy = pltpu.make_async_copy(buffer.at[j], outs[i].at[index], out_sems.at[i, j])
            copy.start()
            departures.append(copy)
    for copy in departures:
        copy.wait()


def _finish_kernel(ids_t, back, token_grad, prob_grad_t):
    total = jnp.sum(back[...].astype(F32), axis=0)
    width = token_grad.shape[1]
    token_grad[...] = total[:, :width].astype(BF16)
    score = total[:, width:].T
    expert = lax.broadcasted_iota(jnp.int32, score.shape, 0)
    found = [
        jnp.sum(jnp.where(expert == ids_t[k : k + 1, :], score, 0.0), axis=0, keepdims=True)
        for k in range(ids_t.shape[0])
    ]
    prob_grad_t[...] = jnp.concatenate(found, axis=0).astype(BF16)


def _in_hbm(values):
    return [pltpu.with_memory_space_constraint(value, pltpu.HBM) for value in values]


def _cost(flops, nbytes):
    return pl.CostEstimate(flops=int(flops), bytes_accessed=int(nbytes), transcendentals=0)


def layer(tokens, out_grad, expert_ids, probs, w_gate, w_up, w_down):
    tok_rows, width = tokens.shape
    top = expert_ids.shape[1]
    local, _, ff = w_gate.shape
    ranks, groups = lax.axis_size("expert"), lax.axis_size("dp")
    experts = local * ranks
    slots = 2 * tok_rows * top // experts
    cols = width // groups
    paired = groups == 4 and ranks == 8 and local % 2 == 0
    pair = 2 if paired else 1
    sets = groups // pair
    own = local // pair
    count = pair * ranks * tok_rows
    rows = pair * ranks * slots
    dp, rank = lax.axis_index("dp"), lax.axis_index("expert")
    core = lax.rem(dp, pair)
    extra = -(-experts // LANES) * LANES
    devices = [(d, e) for d in range(groups) for e in range(ranks)]

    def move(value, target):
        pairs = []
        for d, e in devices:
            to = target(d, e)
            if to is not None:
                pairs.append((d * ranks + e, to[0] * ranks + to[1]))
        return lax.ppermute(value, ("dp", "expert"), pairs)

    def to_core(value):
        return move(value, lambda d, e: (d ^ 1, e))

    def to_chip(value):
        return move(value, lambda d, e: (d ^ 2, e))

    def to_rank(value, offset):
        return move(value, lambda d, e: (d, e ^ offset))

    vmem = pl.BlockSpec(memory_space=pltpu.VMEM)
    smem = pl.BlockSpec(memory_space=pltpu.SMEM)
    hbm = pl.BlockSpec(memory_space=pltpu.HBM)
    limit = pltpu.CompilerParams(vmem_limit_bytes=KERNEL_VMEM)
    packet = pl.pallas_call(
        _pack_kernel,
        out_shape=jax.ShapeDtypeStruct((tok_rows, 2 * width + LANES), BF16),
        in_specs=[vmem] * 4,
        out_specs=vmem,
        name="pack",
    )(tokens, out_grad, expert_ids.T, probs.T)
    half = width // sets
    if paired:
        at = (1 - dp // pair) * half

        def slim(block):
            size = block.shape[:2] + (half,)
            return jnp.concatenate(
                [
                    lax.dynamic_slice(block, (0, 0, at), size),
                    lax.dynamic_slice(block, (0, 0, width + at), size),
                    block[:, :, 2 * width :],
                ],
                axis=2,
            )

        far_z = to_rank(packet, 6)
        mid_z = to_rank(packet, 4)
        low = jnp.stack([packet, to_rank(packet, 1)])
        low = jnp.concatenate([low, to_rank(low, 2)])
        high = jnp.stack([mid_z, far_z])
        relay = to_rank(high, 1)
        high = jnp.stack([high[0], relay[0], high[1], relay[1]])
        far_a = to_chip(slim(low))
        far_b = to_chip(slim(high))
        held = jnp.concatenate([low, high])
        gathered = [held, to_core(held)]
    else:
        gathered = [lax.all_gather(packet, "expert", axis=0)]

    place = jnp.stack([core * own, rank * local + core * own, core, rank]).astype(jnp.int32)

    def fetch(weights, skip, number):
        shape = (number, width, len(weights) * ff)
        return pl.pallas_call(
            functools.partial(_fetch_kernel, skip=skip),
            out_shape=pltpu.VMEM(shape, BF16),
            in_specs=[smem] + [hbm] * len(weights),
            out_specs=vmem,
            scratch_shapes=[pltpu.SemaphoreType.DMA((len(weights), number, SPLIT))],
            compiler_params=pltpu.CompilerParams(vmem_limit_bytes=FETCH_VMEM),
            cost_estimate=_cost(width * ff * own, 4 * own * width * ff),
        )(place, *_in_hbm(weights))

    chunk = own // pair
    wide = [fetch((w_gate, w_up), i * chunk, chunk) for i in range(own // chunk)]
    down = fetch((w_down,), 0, own)
    block = pair * tok_rows
    hidden, chosen, prob = pl.pallas_call(
        functools.partial(
            _hidden_kernel, own=own, rows=rows, top=top, inputs=len(gathered), block=block
        ),
        out_shape=(
            jax.ShapeDtypeStruct((own * rows, 3 * ff), BF16),
            jax.ShapeDtypeStruct((own * rows, count), BF16),
            jax.ShapeDtypeStruct((own, 8, count), F32),
        ),
        in_specs=[smem] + [hbm] * len(gathered) + [vmem] * (len(wide) + 1),
        out_specs=(vmem, vmem, vmem),
        scratch_shapes=[
            pltpu.VMEM((ranks, pair, tok_rows, 2 * width + LANES), BF16),
            pltpu.SemaphoreType.DMA((1, 2)),
        ]
        + [pltpu.VMEM((own * rows, width), BF16)] * 2,
        compiler_params=limit,
        cost_estimate=_cost(6 * own * rows * width * ff, 6 * own * width * ff),
        name="hidden",
    )(place, *gathered, *wide, down)

    if paired:
        sources = gathered + [far_a, far_b, to_core(far_a), to_core(far_b)]
        hidden_far = to_chip(hidden)
        hidden_all = [hidden, to_core(hidden), hidden_far, to_core(hidden_far)]
    else:
        by_owner = gathered[0][:, :, : 2 * width].reshape(ranks, tok_rows, 2, groups, cols)
        by_owner = jnp.moveaxis(by_owner, 3, 0).reshape(groups, ranks, tok_rows, 2 * cols)
        moved = lax.all_to_all(by_owner, "dp", 0, 0, tiled=True)
        metas = lax.all_gather(gathered[0][:, :, 2 * width :], "dp", axis=0)
        sources = [jnp.concatenate([moved[s], metas[s]], axis=2) for s in range(sets)]
        spread = lax.all_gather(hidden, "dp", axis=0)
        hidden_all = [spread[s] for s in range(sets)]

    kernel = functools.partial(
        _return_kernel, own=own, rows=rows, block=block if paired else None
    )
    piece = jax.ShapeDtypeStruct((ranks, tok_rows, width + extra), BF16)
    parts = pl.pallas_call(
        kernel,
        out_shape=(piece,) * pair,
        in_specs=[smem] + [vmem] * (3 + len(wide)),
        out_specs=(vmem,) * pair,
        scratch_shapes=[pltpu.VMEM((own * rows, width), BF16)],
        compiler_params=limit,
        cost_estimate=_cost(8 * own * rows * width * ff, 4 * own * width * ff),
        name="contributions",
    )(place, hidden, chosen, prob, *wide)

    if paired:
        theirs = to_core(parts[1])
        summed = (parts[0].astype(F32) + theirs.astype(F32)).astype(BF16)
    else:
        summed = parts[0]
    back = lax.all_to_all(summed, "expert", 0, 0, tiled=True)
    place_all = jnp.stack([core * own, rank * local, dp, core]).astype(jnp.int32)
    shape = jax.ShapeDtypeStruct((local, cols, ff), F32)
    hidden_all = [value.reshape(own, rows, 3 * ff) for value in hidden_all]
    gate_grad, up_grad, down_grad = pl.pallas_call(
        functools.partial(
            _weights_kernel,
            local=local,
            rows=rows,
            top=top,
            sets=sets,
            halves=pair,
            block=block,
            half=half,
            ff=ff,
            inputs=len(sources),
        ),
        out_shape=(shape, shape, shape),
        in_specs=[smem] + [hbm] * (len(sources) + len(hidden_all)),
        out_specs=(hbm, hbm, hbm),
        scratch_shapes=[
            pltpu.VMEM((sets, ranks, pair, tok_rows, LANES), BF16),
            pltpu.VMEM((sets, ranks, pair, tok_rows, cols), BF16),
            pltpu.VMEM((sets, ranks, pair, tok_rows, cols), BF16),
            pltpu.SemaphoreType.DMA((sets, 3, 4)),
            pltpu.VMEM((local, sets * rows, 3 * ff), BF16),
        ]
        + [pltpu.VMEM((local, cols, ff), F32)] * 3
        + [pltpu.SemaphoreType.DMA((pair, sets)), pltpu.SemaphoreType.DMA((3, local))],
        compiler_params=pltpu.CompilerParams(vmem_limit_bytes=WIDE_VMEM),
        cost_estimate=_cost(6 * local * sets * rows * cols * ff, 12 * local * cols * ff),
        name="weight_grads",
    )(place_all, *sources, *hidden_all)
    token_grad, prob_grad_t = pl.pallas_call(
        _finish_kernel,
        out_shape=(
            jax.ShapeDtypeStruct((tok_rows, width), BF16),
            jax.ShapeDtypeStruct((top, tok_rows), BF16),
        ),
        in_specs=[vmem] * 2,
        out_specs=(vmem, vmem),
        name="finish",
    )(expert_ids.T, back)
    prob_grad = prob_grad_t.T
    return (token_grad, prob_grad, gate_grad, up_grad, down_grad)


def solution(mesh):
    placed = (
        P(("dp", "expert"), None),
        P(("dp", "expert"), None),
        P(("dp", "expert"), None),
        P(("dp", "expert"), None),
        P("expert", None, None),
        P("expert", None, None),
        P("expert", None, None),
    )
    return jax.shard_map(
        layer,
        mesh=mesh,
        in_specs=placed,
        out_specs=(
            P(("dp", "expert"), None),
            P(("dp", "expert"), None),
            P("expert", "dp", None),
            P("expert", "dp", None),
            P("expert", "dp", None),
        ),
        check_vma=False,
    )
```
